32 devices in a mesh: dp: 4 (over z), mp: 8 (over y, x, core).
Axes of the slice: x: 2, y: 2, z: 4, core: 2. Of those that a mesh axis runs over, the one named last changes fastest.
Arguments:
- tokens: bfloat16 [4096, 4096], P('dp', 'mp'), may hold values from -6 to 6
- decay: float32 [4096, 16], P('dp'), may hold values from 0.75 to 1, as said below
- state: float32 [128, 256, 8192], P('dp', None, 'mp'), may hold values from -24 to 24
- w_query: bfloat16 [4096, 4096], P(None, 'mp'), may hold values from -0.09375 to 0.09375
- w_key: bfloat16 [4096, 4096], P(None, 'mp'), may hold values from -0.09375 to 0.09375
- w_value: bfloat16 [4096, 8192], P(None, 'mp'), may hold values from -0.09375 to 0.09375
- w_gate: bfloat16 [4096, 8192], P(None, 'mp'), may hold values from -0.09375 to 0.09375
- w_out: bfloat16 [8192, 4096], P('mp'), may hold values from -0.09375 to 0.09375
- norm_gain: float32 [8192], P('mp'), may hold values from 0.25 to 1.75
Outputs:
- layer_out: bfloat16 [4096, 4096], P('dp', 'mp')
- new_state: float32 [128, 256, 8192], P('dp', None, 'mp')
The draws below stay inside these ranges and needn't reach their ends.
Inputs may be any that keep to these rules, and one draw needn't show every extreme that they name: `decay`: each head has its own base rate over all tokens, varied somewhat from token to token.
All inputs are finite; a program needn't handle non-finite values.
Results may differ from the reference program's by a relative error of at most 0.0071.
Values may be sent and summed in bfloat16 or wider, within the bound.
A program may use at most 256 MiB of HBM per device.

```python
import jax
import jax.numpy as jnp
from jax import lax

D = 4096
H = 16
HEAD = 256
VHEAD = 512
NEW = 32
BATCH = 128
TOKENS = 4096


def draw_decay(key, part):
    base_key, jitter_key = jax.random.split(key)
    base_low = 0.85
    jitter_low = 0.93
    base_rate = jnp.exp(jax.random.uniform(base_key, (H,), jnp.float32, jnp.log(base_low), jnp.log(0.999)))
    jitter = jax.random.uniform(jitter_key, (TOKENS, H), jnp.float32, jitter_low, 1.0)
    return base_rate[None, :] * jitter


def with_spikes(result, key, source, target, parts, factor):
    owner, partner = [(jnp.arange(result.shape[position]) // (result.shape[position] // parts)).reshape([-1 if axis == position else 1 for axis in range(result.ndim)]) for position in (source, target)]
    chosen = jax.random.permutation(key, parts)[partner]
    strong = (owner == chosen) | (owner == (partner + parts // 2) % parts)
    return jnp.where(strong, factor * result, result)


def block_levels(rng, dims, shards, low, largest):
    level = 1.0
    for position, shards_of in shards:
        heights = jax.random.uniform(jax.random.fold_in(jax.random.fold_in(rng, 6), position), (shards_of,), jnp.float32, low / len(shards), largest / len(shards))
        level = level * jnp.repeat(jnp.exp(heights), dims[position] // shards_of).reshape((-1,) + (1,) * (len(dims) - 1 - position))
    return level


def gaussian(rng, shape, scale, most, cuts=(), held_as=jnp.bfloat16):
    values = scale * jax.random.normal(rng, shape, jnp.float32)
    if cuts:
        values = values * block_levels(rng, shape, cuts, -0.22, 0.18)
    return jnp.clip(values, -most, most).astype(held_as)


def bell_draw_with(own_key, shape, width, most, pieces, heavy, held_as=jnp.bfloat16):
    result = width * jax.random.normal(own_key, shape, jnp.float32)
    if pieces:
        result = result * block_levels(own_key, shape, pieces, -0.22, 0.18)
    return jnp.clip(with_spikes(result, jax.random.fold_in(own_key, 3), *heavy), -most, most).astype(held_as)


def setup_inputs(seed: int = 0) -> dict:
    arg_keys = jax.random.split(jax.random.key(seed), 10)
    return {
        "tokens": gaussian(arg_keys[0], (TOKENS, D), 1.0, 6.0, ((0, 4), (1, 8))),
        "decay": draw_decay(jax.random.fold_in(arg_keys[9], 71), 0),
        "state": gaussian(arg_keys[2], (BATCH, HEAD, H * VHEAD), 4.0, 24.0, ((0, 4), (2, 8)), jnp.float32),
        "w_query": gaussian(arg_keys[3], (D, H * HEAD), D ** -0.5, 0.09375, ((1, 8),)),
        "w_key": gaussian(arg_keys[4], (D, H * HEAD), D ** -0.5, 0.09375, ((1, 8),)),
        "w_value": gaussian(arg_keys[5], (D, H * VHEAD), D ** -0.5, 0.09375, ((1, 8),)),
        "w_gate": gaussian(arg_keys[6], (D, H * VHEAD), D ** -0.5, 0.09375, ((1, 8),)),
        "w_out": bell_draw_with(arg_keys[7], (H * VHEAD, D), (H * VHEAD) ** -0.5, 0.09375, ((0, 8),), (0, 1, 8, 2.0)),
        "norm_gain": jnp.clip(1.0 + 0.15 * jax.random.normal(arg_keys[8], (H * VHEAD,), jnp.float32), 0.25, 1.75),
    }


EPS = 0.1

def one_sequence(packed):
    query, key_proj, value_proj, decay_rates, old_state = packed
    highest = lax.Precision.HIGHEST
    log_cumul = jnp.cumsum(jnp.log(decay_rates), axis=0)
    from_state = jnp.einsum('nhk,khv->nhv', query.astype(jnp.float32), old_state, precision=highest)
    scores = jnp.einsum('nhk,mhk->hnm', query.astype(jnp.float32), key_proj.astype(jnp.float32), precision=highest)
    along = log_cumul.T
    log_gap = along[:, :, None] - along[:, None, :]
    causal = jnp.arange(NEW)[:, None] >= jnp.arange(NEW)[None, :]
    factor = jnp.where(causal, jnp.exp(jnp.where(causal, log_gap, 0.0)), 0.0)
    weights = (scores * factor).astype(jnp.bfloat16)
    in_block = jnp.einsum('hnm,mhv->nhv', weights.astype(jnp.float32), value_proj.astype(jnp.float32), precision=highest)
    retained = jnp.exp(log_cumul)[:, :, None] * from_state + in_block
    final_log = log_cumul[-1]
    carry_scale = jnp.exp(final_log[None, :] - log_cumul)
    decayed_keys = key_proj.astype(jnp.float32) * carry_scale[:, :, None]
    fresh = jnp.einsum('nhk,nhv->khv', decayed_keys, value_proj.astype(jnp.float32), precision=highest)
    new_state = jnp.exp(final_log)[None, :, None] * old_state + fresh
    return (retained, new_state)

def reference(tokens, decay, state, w_query, w_key, w_value, w_gate, w_out, norm_gain):
    query = (jnp.dot(tokens, w_query, preferred_element_type=jnp.float32) * HEAD ** (-0.5)).astype(jnp.bfloat16)
    key_proj = jnp.dot(tokens, w_key, preferred_element_type=jnp.float32).astype(jnp.bfloat16)
    value_proj = jnp.dot(tokens, w_value, preferred_element_type=jnp.float32).astype(jnp.bfloat16)
    gate_proj = jnp.dot(tokens, w_gate, preferred_element_type=jnp.float32)
    packed = (query.reshape(BATCH, NEW, H, HEAD), key_proj.reshape(BATCH, NEW, H, HEAD), value_proj.reshape(BATCH, NEW, H, VHEAD), decay.reshape(BATCH, NEW, H), state.reshape(BATCH, HEAD, H, VHEAD))
    retained, new_state = lax.map(one_sequence, packed)
    retained = retained.reshape(TOKENS, H, VHEAD)
    centre = lax.optimization_barrier(jnp.mean(retained, axis=-1))
    deviation = retained - centre[..., None]
    variance = lax.optimization_barrier(jnp.mean(deviation * deviation, axis=-1))
    normed = deviation * lax.rsqrt(variance + EPS)[..., None]
    gated_out = (normed.reshape(TOKENS, H * VHEAD) * norm_gain * jax.nn.silu(gate_proj)).astype(jnp.bfloat16)
    layer_out = jnp.dot(gated_out, w_out, preferred_element_type=jnp.float32).astype(jnp.bfloat16)
    return (layer_out, new_state.reshape(BATCH, HEAD, H * VHEAD))
```

```python
import functools

import jax
import jax.numpy as jnp
from jax import lax
from jax.experimental import pallas as pl
from jax.experimental.pallas import tpu as pltpu
from jax.sharding import PartitionSpec as P

HEAD = 256
VHEAD = 512
NEW = 32


EPS = 0.1


def partner(shard, axis, bit):
    return lax.ppermute(shard, axis, [(i, i ^ 1 << bit) for i in range(lax.axis_size(axis))])


def split_heads(tokens, decay, state, w_query, w_key, w_value, w_gate, w_out, norm_gain):
    highest = lax.Precision.HIGHEST
    tok_rows = tokens.shape[0]
    qk_columns = w_query.shape[1]
    v_columns = w_value.shape[1]
    head_span = max(1, HEAD // qk_columns)
    groups = max(1, qk_columns // HEAD)
    qk_width = qk_columns // groups
    v_width = v_columns // groups
    sequences = tok_rows // NEW
    bit_count = head_span.bit_length() - 1
    device_index = lax.axis_index("mp")
    first_head = device_index * qk_columns // HEAD
    qk_zeros = jnp.zeros((tok_rows, qk_columns), jnp.float32)
    v_zeros = jnp.zeros((tok_rows, v_columns), jnp.float32)
    carried = (qk_zeros, qk_zeros, v_zeros, v_zeros)
    segment = lax.all_gather(tokens, "mp", axis=1, tiled=True)
    updated = []
    for running, weight in zip(carried, (w_query, w_key, w_value, w_gate)):
        updated.append(jnp.dot(segment, weight, preferred_element_type=jnp.float32))
    query, key_proj, value_proj, gate_proj = tuple(updated)
    query = (query * HEAD ** (-0.5)).astype(jnp.bfloat16).reshape(tok_rows, groups, qk_width)
    key_proj = key_proj.astype(jnp.bfloat16).reshape(tok_rows, groups, qk_width)
    value_proj = value_proj.astype(jnp.bfloat16)
    for bit_number in range(bit_count):
        other_query, other_key = partner((query, key_proj), "mp", bit_number)
        upper_half = device_index >> bit_number & 1 == 1
        query = jnp.where(
            upper_half,
            jnp.concatenate([other_query, query], 2),
            jnp.concatenate([query, other_query], 2),
        )
        key_proj = jnp.where(
            upper_half,
            jnp.concatenate([other_key, key_proj], 2),
            jnp.concatenate([key_proj, other_key], 2),
        )
    query_block = query.reshape(sequences, NEW, groups, HEAD)
    key_block = key_proj.reshape(sequences, NEW, groups, HEAD)
    value_block = value_proj.reshape(sequences, NEW, groups, v_width)
    decay_rates = lax.dynamic_slice_in_dim(decay, first_head, groups, 1).reshape(
        sequences, NEW, groups
    )
    log_cumul = jnp.cumsum(jnp.log(decay_rates), axis=1)
    old_state = state.reshape(sequences, HEAD, groups, v_width)
    from_state = jnp.einsum(
        "bngk,bkgv->bngv", query_block.astype(jnp.float32), old_state, precision=highest
    )
    scores = jnp.einsum(
        "bngk,bmgk->bgnm", query_block, key_block, preferred_element_type=jnp.float32
    )
    along = jnp.transpose(log_cumul, (0, 2, 1))
    log_gap = along[:, :, :, None] - along[:, :, None, :]
    causal = jnp.arange(NEW)[:, None] >= jnp.arange(NEW)[None, :]
    factor = jnp.where(causal, jnp.exp(jnp.where(causal, log_gap, 0.0)), 0.0)
    weights = (scores * factor).astype(jnp.bfloat16)
    in_block = jnp.einsum(
        "bgnm,bmgv->bngv", weights, value_block, preferred_element_type=jnp.float32
    )
    retained = jnp.exp(log_cumul)[..., None] * from_state + in_block
    final_log = log_cumul[:, -1, :]
    carry_scale = jnp.exp(final_log[:, None, :] - log_cumul)
    decayed_keys = key_block.astype(jnp.float32) * carry_scale[..., None]
    fresh = jnp.einsum(
        "bngk,bngv->bkgv", decayed_keys, value_block.astype(jnp.float32), precision=highest
    )
    new_state = jnp.exp(final_log)[:, None, :, None] * old_state + fresh
    new_state = new_state.reshape(sequences, HEAD, v_columns)
    retained = retained.reshape(tok_rows, groups, v_width)
    running = jnp.sum(retained, axis=-1)
    squares = jnp.sum(retained * retained, axis=-1)
    for bit_number in range(bit_count):
        other_sum, other_square = partner((running, squares), "mp", bit_number)
        running = running + other_sum
        squares = squares + other_square
    centre = running / VHEAD
    variance = squares / VHEAD - centre * centre
    deviation = retained - centre[..., None]
    normed = deviation * lax.rsqrt(variance + EPS)[..., None]
    gated_out = (normed.reshape(tok_rows, v_columns) * norm_gain * jax.nn.silu(gate_proj)).astype(
        jnp.bfloat16
    )
    partial_terms = jnp.dot(gated_out, w_out, preferred_element_type=jnp.float32)
    layer_out = lax.psum_scatter(partial_terms, "mp", scatter_dimension=1, tiled=True).astype(
        jnp.bfloat16
    )
    return (layer_out, new_state)


CHUNKS = 8
EXCHANGED = 5
TILE = 512
PER_STEP = 2


def partners(device):
    core = device % 2
    across_x = device + 2 - 4 * ((device // 2) % 2)
    across_y = device + 4 - 8 * (device // 4)
    near = across_x + core * (across_y - across_x)
    far = across_y + core * (across_x - across_y)
    return near, far, across_x + across_y - device, device + 1 - 2 * core


def meet(devices):
    barrier = pltpu.get_barrier_semaphore()
    for device in devices:
        pl.semaphore_signal(
            barrier, inc=1, device_id={"mp": device}, device_id_type=pl.DeviceIdType.MESH
        )
    pl.semaphore_wait(barrier, len(devices))


def remote(source, target, send, recv, device):
    return pltpu.make_async_remote_copy(
        src_ref=source,
        dst_ref=target,
        send_sem=send,
        recv_sem=recv,
        device_id={"mp": device},
        device_id_type=pl.DeviceIdType.MESH,
    )


def fused_kernel(
    chunks,
    reduced,
    groups,
    tokens,
    w_query,
    w_key,
    w_value,
    w_gate,
    w_out,
    state,
    c_col,
    c_row,
    gain,
    key_out,
    value_out,
    layer_out,
    own_out,
    near_out,
    far_out,
    diag_out,
    gathered,
    wq,
    wk,
    wv,
    wg,
    wo,
    q_held,
    k_held,
    v_held,
    g_held,
    s_held,
    gated,
    to_sibling,
    from_sibling,
    outgoing,
    incoming,
    total,
    pending,
    finished,
    load_sem,
    state_sem,
    kv_sem,
    out_sem,
    send,
    recv,
    sum_send,
    sum_recv,
):
    me = lax.axis_index("mp")
    near, far, diagonal, sibling = partners(me)
    sib_near, sib_far, sib_diagonal, _ = partners(sibling)
    mine = (me, near, far, diagonal)
    theirs = (sibling, sib_near, sib_far, sib_diagonal)
    rows, width = tokens.shape
    size = rows // chunks
    sequences = size // NEW
    vw = w_value.shape[1] // groups

    def at(r):
        return pl.ds(pl.multiple_of(r * size, size), size)

    def span(device):
        return pl.ds(pl.multiple_of(device * width, width), width)

    def copy(lane, source, target, r):
        there = gathered.at[at(r), span(source)]
        return remote(there, there, send.at[lane, r], recv.at[lane, r], target)

    def swap(j, r):
        return remote(
            to_sibling.at[lax.rem(r, 2), j],
            from_sibling.at[j, at(r), :],
            sum_send.at[j, r],
            sum_recv.at[j, r],
            sibling,
        )

    def hop(lane, r):
        return remote(
            outgoing.at[lane, at(r), :],
            incoming.at[lane, at(r), :],
            sum_send.at[4 + lane, r],
            sum_recv.at[4 + lane, r],
            near if lane == 0 else far,
        )

    own = pltpu.make_async_copy(tokens, gathered.at[:, span(me)], load_sem.at[0])
    own.start()
    loads = [
        pltpu.make_async_copy(source, held, load_sem.at[1 + n])
        for n, (source, held) in enumerate(
            ((w_query, wq), (w_key, wk), (w_value, wv), (w_gate, wg), (w_out, wo))
        )
    ]
    for load in loads:
        load.start()

    def load_state(r):
        first = pl.multiple_of(r * sequences, sequences)
        return pltpu.make_async_copy(
            state.at[pl.ds(first, sequences)], s_held, state_sem.at[0]
        )

    def store_key(r):
        return pltpu.make_async_copy(
            k_held.at[lax.rem(r, 2)], key_out.at[at(r), :], kv_sem.at[0, r]
        )

    def store_value(r):
        return pltpu.make_async_copy(
            v_held.at[lax.rem(r, 2)], value_out.at[at(r), :], kv_sem.at[1, r]
        )

    def store_layer(r):
        return pltpu.make_async_copy(
            finished.at[at(r), :], layer_out.at[at(r), :], out_sem.at[0, r]
        )

    def store_shares(r):
        there = at(r - reduced)
        return [pltpu.make_async_copy(total.at[at(r), :], own_out.at[there, :], out_sem.at[0, r])] + [
            pltpu.make_async_copy(
                outgoing.at[lane, at(r), :], target.at[there, :], out_sem.at[1 + lane, r]
            )
            for lane, target in enumerate((near_out, far_out, diag_out))
        ]

    meet((near, far, sibling))
    own.wait()

    def pass_near(r):
        copy(0, near, near, r).wait_recv()
        copy(2, near, far, r).start()
        copy(4, near, sibling, r).start()

    def pass_far(r):
        copy(1, far, far, r).wait_recv()
        copy(5, far, sibling, r).start()

    def pass_diagonal(r):
        copy(2, diagonal, far, r).wait_recv()
        copy(6, diagonal, sibling, r).start()

    copy(0, me, near, 0).start()
    copy(1, me, far, 0).start()
    copy(3, me, sibling, 0).start()
    copy(0, me, near, 1).start()
    pass_near(0)
    copy(1, me, far, 1).start()
    copy(3, me, sibling, 1).start()
    copy(0, me, near, 2).start()
    pass_far(0)
    pass_diagonal(0)
    pass_near(1)
    copy(1, me, far, 2).start()
    copy(3, me, sibling, 2).start()
    pass_far(1)

    place = lax.broadcasted_iota(jnp.int32, (size, size), 0)
    other = lax.broadcasted_iota(jnp.int32, (size, size), 1)
    causal = (place >= other) & (place // NEW == other // NEW)

    def project(r, weight, col, stop):
        return jnp.dot(
            gathered[at(r), :], weight[:, col:stop], preferred_element_type=jnp.float32
        )

    def share(dest):
        return jnp.dot(gated[...], wo[:, span(dest)], preferred_element_type=jnp.float32)

    def relay(r):
        hop(2, r).wait_recv()
        part = pending[lax.rem(r, 2)] + incoming[2, at(r), :].astype(jnp.float32)
        outgoing[0, at(r), :] = part.astype(jnp.bfloat16)
        hop(0, r).start()

    def finish(r):
        hop(1, r).wait_recv()
        hop(0, r).wait_recv()
        finished[at(r), :] = (
            total[at(r), :]
            + incoming[0, at(r), :].astype(jnp.float32)
            + incoming[1, at(r), :].astype(jnp.float32)
        ).astype(jnp.bfloat16)
        store_layer(r).start()

    def step(r, carry):
        slot = lax.rem(r, 2)
        load_state(r).start()
        for lane, source in ((3, sibling), (4, sib_near), (5, sib_far), (6, sib_diagonal)):
            copy(lane, source, sibling, r).wait_recv()

        @pl.when(r == 0)
        def _():
            loads[0].wait()
            loads[1].wait()

        @pl.when(r >= 2)
        def _():
            store_key(r - 2).wait()
            store_value(r - 2).wait()

        for col in range(0, wq.shape[1], TILE):
            stop = min(col + TILE, wq.shape[1])
            q_held[:, col:stop] = (project(r, wq, col, stop) * HEAD ** (-0.5)).astype(jnp.bfloat16)
            k_held[slot, :, col:stop] = project(r, wk, col, stop).astype(jnp.bfloat16)
        store_key(r).start()

        @pl.when(r + 1 < chunks)
        def _():
            pass_diagonal(r + 1)

        @pl.when((r >= 1) & (r - 1 < reduced))
        def _():
            relay(r - 1)

        @pl.when(r == 0)
        def _():
            loads[2].wait()
            loads[3].wait()

        for col in range(0, wv.shape[1], TILE):
            stop = min(col + TILE, wv.shape[1])
            v_held[slot, :, col:stop] = project(r, wv, col, stop).astype(jnp.bfloat16)
        store_value(r).start()

        @pl.when(r + 2 < chunks)
        def _():
            pass_near(r + 2)
            pass_far(r + 2)

        @pl.when(r + 3 < chunks)
        def _():
            copy(0, me, near, r + 3).start()
            copy(1, me, far, r + 3).start()
            copy(3, me, sibling, r + 3).start()

        for col in range(0, wg.shape[1], TILE):
            stop = min(col + TILE, wg.shape[1])
            gates = project(r, wg, col, stop)
            g_held[:, col:stop] = gain[:, col:stop] * (gates / (1.0 + jnp.exp(-gates)))

        load_state(r).wait()
        for g in range(groups):
            vs = slice(g * vw, (g + 1) * vw)
            ks = slice(g * HEAD, (g + 1) * HEAD)
            query, key, value = q_held[:, ks], k_held[slot, :, ks], v_held[slot, :, vs]
            col = c_col[at(r), g : g + 1]
            row = c_row[r, g : g + 1, :]
            scores = lax.dot_general(
                query, key, (((1,), (1,)), ((), ())), preferred_element_type=jnp.float32
            )
            factor = jnp.where(causal, jnp.exp(jnp.where(causal, col - row, 0.0)), 0.0)
            weights = (scores * factor).astype(jnp.bfloat16)
            from_state = jnp.concatenate(
                [
                    jnp.dot(
                        query[s * NEW : (s + 1) * NEW],
                        s_held[s, :, vs].astype(jnp.bfloat16),
                        preferred_element_type=jnp.float32,
                    )
                    for s in range(sequences)
                ],
                axis=0,
            )
            in_block = jnp.dot(weights, value, preferred_element_type=jnp.float32)
            retained = jnp.exp(col) * from_state + in_block
            centre = jnp.mean(retained, axis=1, keepdims=True)
            deviation = retained - centre
            variance = jnp.mean(deviation * deviation, axis=1, keepdims=True)
            normed = deviation * lax.rsqrt(variance + EPS)
            gated[:, vs] = (normed * g_held[:, vs]).astype(jnp.bfloat16)

        @pl.when(r == 0)
        def _():
            loads[4].wait()

        for j in (3, 2, 1, 0):

            @pl.when(r >= 2)
            def _():
                swap(j, r - 2).wait_send()

            to_sibling[slot, j] = share(theirs[j]).astype(jnp.bfloat16)
            swap(j, r).start()

        @pl.when((r >= 2) & (r - 2 < reduced))
        def _():
            finish(r - 2)

        for j in (3, 2, 1, 0):
            part = share(mine[j])
            swap(j, r).wait_recv()
            part = part + from_sibling[j, at(r), :].astype(jnp.float32)
            if j >= 2:
                outgoing[j - 1, at(r), :] = part.astype(jnp.bfloat16)

                @pl.when(r < reduced)
                def _():
                    hop(j - 1, r).start()
            elif j == 1:
                pending[slot] = part

                @pl.when(r >= reduced)
                def _():
                    outgoing[0, at(r), :] = part.astype(jnp.bfloat16)
            else:
                total[at(r), :] = part

        @pl.when(r >= reduced)
        def _():
            for store in store_shares(r):
                store.start()

        return carry

    lax.fori_loop(0, chunks, step, 0)
    if reduced == chunks:
        relay(reduced - 1)
    for r in (chunks - 2, chunks - 1):
        if r < reduced:
            finish(r)

    def drain(r, carry):
        for lane, (source, target) in enumerate(
            (
                (me, near),
                (me, far),
                (near, far),
                (me, sibling),
                (near, sibling),
                (far, sibling),
                (diagonal, sibling),
            )
        ):
            copy(lane, source, target, r).wait_send()

        @pl.when(r >= chunks - 2)
        def _():
            store_key(r).wait()
            store_value(r).wait()
            for j in range(4):
                swap(j, r).wait_send()

        @pl.when(r < reduced)
        def _():
            for lane in range(3):
                hop(lane, r).wait_send()
            store_layer(r).wait()

        @pl.when(r >= reduced)
        def _():
            for store in store_shares(r):
                store.wait()

        return carry

    lax.fori_loop(0, chunks, drain, 0)


def fused(tokens, w_query, w_key, w_value, w_gate, w_out, state, c_col, c_row, gain):
    rows, width = tokens.shape
    depth, qk = w_query.shape
    vc = w_value.shape[1]
    chunks, reduced = CHUNKS, EXCHANGED
    size = rows // chunks
    groups = c_col.shape[1]
    kept = reduced * size
    rest = rows - kept
    anywhere = pl.BlockSpec(memory_space=pl.ANY)
    vmem = pl.BlockSpec(memory_space=pltpu.VMEM)
    narrow = jnp.bfloat16
    wide = jnp.float32
    shapes = [
        ((rows, qk), narrow),
        ((rows, vc), narrow),
        ((kept, width), narrow),
        ((rest, width), wide),
        ((rest, width), narrow),
        ((rest, width), narrow),
        ((rest, width), narrow),
    ]
    return pl.pallas_call(
        functools.partial(fused_kernel, chunks, reduced, groups),
        in_specs=[anywhere] * 7 + [vmem] * 3,
        out_specs=[anywhere] * len(shapes),
        out_shape=[jax.ShapeDtypeStruct(*shape) for shape in shapes],
        scratch_shapes=[
            pltpu.VMEM((rows, depth), narrow),
            pltpu.VMEM((depth, qk), narrow),
            pltpu.VMEM((depth, qk), narrow),
            pltpu.VMEM((depth, vc), narrow),
            pltpu.VMEM((depth, vc), narrow),
            pltpu.VMEM(w_out.shape, narrow),
            pltpu.VMEM((size, qk), narrow),
            pltpu.VMEM((2, size, qk), narrow),
            pltpu.VMEM((2, size, vc), narrow),
            pltpu.VMEM((size, vc), wide),
            pltpu.VMEM((size // NEW,) + state.shape[1:], wide),
            pltpu.VMEM((size, vc), narrow),
            pltpu.VMEM((2, 4, size, width), narrow),
            pltpu.VMEM((4, rows, width), narrow),
            pltpu.VMEM((3, rows, width), narrow),
            pltpu.VMEM((3, kept, width), narrow),
            pltpu.VMEM((rows, width), wide),
            pltpu.VMEM((2, size, width), wide),
            pltpu.VMEM((kept, width), narrow),
            pltpu.SemaphoreType.DMA((6,)),
            pltpu.SemaphoreType.DMA((1,)),
            pltpu.SemaphoreType.DMA((2, chunks)),
            pltpu.SemaphoreType.DMA((4, chunks)),
            pltpu.SemaphoreType.DMA((7, chunks)),
            pltpu.SemaphoreType.DMA((7, chunks)),
            pltpu.SemaphoreType.DMA((7, chunks)),
            pltpu.SemaphoreType.DMA((7, chunks)),
        ],
        compiler_params=pltpu.CompilerParams(
            collective_id=0, has_side_effects=True, vmem_limit_bytes=67043328
        ),
        cost_estimate=pl.CostEstimate(
            flops=2 * rows * depth * (2 * qk + 3 * vc),
            bytes_accessed=4 * state.size,
            transcendentals=rows * vc,
        ),
    )(tokens, w_query, w_key, w_value, w_gate, w_out, state, c_col, c_row, gain)


def update_step(per_step, groups, c_col, k, v, state, new_state):
    vw = v.shape[1] // groups
    for s in range(per_step):
        at = slice(s * NEW, (s + 1) * NEW)
        for g in range(groups):
            vs = slice(g * vw, (g + 1) * vw)
            col = c_col[at, g : g + 1]
            last = col[NEW - 1 : NEW, :]
            key = k[at, g * HEAD : (g + 1) * HEAD].astype(jnp.float32)
            scaled = (key * jnp.exp(last - col)).astype(jnp.bfloat16)
            fresh = lax.dot_general(
                scaled, v[at, vs], (((0,), (0,)), ((), ())), preferred_element_type=jnp.float32
            )
            new_state[s, :, vs] = jnp.exp(last) * state[s, :, vs] + fresh


def update_state(c_col, k, v, state):
    rows, groups = c_col.shape
    sequences = rows // NEW
    per_step = PER_STEP if sequences % PER_STEP == 0 else 1
    by_row = lambda width: pl.BlockSpec((per_step * NEW, width), lambda i: (i, 0))
    state_spec = pl.BlockSpec((per_step,) + state.shape[1:], lambda i: (i, 0, 0))
    return pl.pallas_call(
        functools.partial(update_step, per_step, groups),
        grid=(sequences // per_step,),
        in_specs=[by_row(groups), by_row(k.shape[1]), by_row(v.shape[1]), state_spec],
        out_specs=state_spec,
        out_shape=jax.ShapeDtypeStruct(state.shape, jnp.float32),
        compiler_params=pltpu.CompilerParams(
            dimension_semantics=("arbitrary",), vmem_limit_bytes=60 << 20
        ),
        cost_estimate=pl.CostEstimate(
            flops=2 * rows * HEAD * v.shape[1],
            bytes_accessed=8 * state.size,
            transcendentals=rows,
        ),
    )(c_col, k, v, state)


def whole_heads(tokens, decay, state, w_query, w_key, w_value, w_gate, w_out, norm_gain):
    tok_rows = tokens.shape[0]
    groups = w_query.shape[1] // HEAD
    sequences = tok_rows // NEW
    first_head = lax.axis_index("mp") * groups
    logs = jnp.log(lax.dynamic_slice_in_dim(decay, first_head, groups, 1))
    logs = logs.reshape(sequences, NEW, groups)
    causal = jnp.arange(NEW)[:, None] >= jnp.arange(NEW)[None, :]
    cumul = jnp.sum(jnp.where(causal[None, :, :, None], logs[:, None], 0.0), axis=2)
    c_col = cumul.reshape(tok_rows, groups)
    c_row = jnp.transpose(cumul.reshape(CHUNKS, tok_rows // CHUNKS, groups), (0, 2, 1))
    key_proj, value_proj, reduced, own, *shares = fused(
        tokens,
        w_query,
        w_key,
        w_value,
        w_gate,
        w_out,
        state,
        c_col,
        c_row,
        norm_gain.reshape(1, -1),
    )
    devices = range(lax.axis_size("mp"))
    for n, share in enumerate(shares):
        pairs = [(device, partners(device)[n]) for device in devices]
        own = own + lax.ppermute(share, "mp", pairs).astype(jnp.float32)
    layer_out = jnp.concatenate([reduced, own.astype(jnp.bfloat16)])
    return (layer_out, update_state(c_col, key_proj, value_proj, state))


def per_device(tokens, decay, state, w_query, *rest):
    whole = w_query.shape[1] % HEAD == 0 and lax.axis_size("mp") == 8
    path = whole_heads if whole else split_heads
    return path(tokens, decay, state, w_query, *rest)


def solution(mesh):
    placed = (
        P("dp", "mp"),
        P("dp", None),
        P("dp", None, "mp"),
        P(None, "mp"),
        P(None, "mp"),
        P(None, "mp"),
        P(None, "mp"),
        P("mp", None),
        P("mp"),
    )
    return jax.shard_map(
        per_device,
        mesh=mesh,
        in_specs=placed,
        out_specs=(P("dp", "mp"), P("dp", None, "mp")),
        check_vma=False,
    )
```

```python
import functools

import jax
import jax.numpy as jnp
from jax import lax
from jax.experimental import pallas as pl
from jax.experimental.pallas import tpu as pltpu
from jax.sharding import PartitionSpec as P

HEAD = 256
VHEAD = 512
NEW = 32


EPS = 0.1


def partner(shard, axis, bit):
    return lax.ppermute(shard, axis, [(i, i ^ 1 << bit) for i in range(lax.axis_size(axis))])


def split_heads(tokens, decay, state, w_query, w_key, w_value, w_gate, w_out, norm_gain):
    highest = lax.Precision.HIGHEST
    tok_rows = tokens.shape[0]
    qk_columns = w_query.shape[1]
    v_columns = w_value.shape[1]
    head_span = max(1, HEAD // qk_columns)
    groups = max(1, qk_columns // HEAD)
    qk_width = qk_columns // groups
    v_width = v_columns // groups
    sequences = tok_rows // NEW
    bit_count = head_span.bit_length() - 1
    device_index = lax.axis_index("mp")
    first_head = device_index * qk_columns // HEAD
    qk_zeros = jnp.zeros((tok_rows, qk_columns), jnp.float32)
    v_zeros = jnp.zeros((tok_rows, v_columns), jnp.float32)
    carried = (qk_zeros, qk_zeros, v_zeros, v_zeros)
    segment = lax.all_gather(tokens, "mp", axis=1, tiled=True)
    updated = []
    for running, weight in zip(carried, (w_query, w_key, w_value, w_gate)):
        updated.append(jnp.dot(segment, weight, preferred_element_type=jnp.float32))
    query, key_proj, value_proj, gate_proj = tuple(updated)
    query = (query * HEAD ** (-0.5)).astype(jnp.bfloat16).reshape(tok_rows, groups, qk_width)
    key_proj = key_proj.astype(jnp.bfloat16).reshape(tok_rows, groups, qk_width)
    value_proj = value_proj.astype(jnp.bfloat16)
    for bit_number in range(bit_count):
        other_query, other_key = partner((query, key_proj), "mp", bit_number)
        upper_half = device_index >> bit_number & 1 == 1
        query = jnp.where(
            upper_half,
            jnp.concatenate([other_query, query], 2),
            jnp.concatenate([query, other_query], 2),
        )
        key_proj = jnp.where(
            upper_half,
            jnp.concatenate([other_key, key_proj], 2),
            jnp.concatenate([key_proj, other_key], 2),
        )
    query_block = query.reshape(sequences, NEW, groups, HEAD)
    key_block = key_proj.reshape(sequences, NEW, groups, HEAD)
    value_block = value_proj.reshape(sequences, NEW, groups, v_width)
    decay_rates = lax.dynamic_slice_in_dim(decay, first_head, groups, 1).reshape(
        sequences, NEW, groups
    )
    log_cumul = jnp.cumsum(jnp.log(decay_rates), axis=1)
    old_state = state.reshape(sequences, HEAD, groups, v_width)
    from_state = jnp.einsum(
        "bngk,bkgv->bngv", query_block.astype(jnp.float32), old_state, precision=highest
    )
    scores = jnp.einsum(
        "bngk,bmgk->bgnm", query_block, key_block, preferred_element_type=jnp.float32
    )
    along = jnp.transpose(log_cumul, (0, 2, 1))
    log_gap = along[:, :, :, None] - along[:, :, None, :]
    causal = jnp.arange(NEW)[:, None] >= jnp.arange(NEW)[None, :]
    factor = jnp.where(causal, jnp.exp(jnp.where(causal, log_gap, 0.0)), 0.0)
    weights = (scores * factor).astype(jnp.bfloat16)
    in_block = jnp.einsum(
        "bgnm,bmgv->bngv", weights, value_block, preferred_element_type=jnp.float32
    )
    retained = jnp.exp(log_cumul)[..., None] * from_state + in_block
    final_log = log_cumul[:, -1, :]
    carry_scale = jnp.exp(final_log[:, None, :] - log_cumul)
    decayed_keys = key_block.astype(jnp.float32) * carry_scale[..., None]
    fresh = jnp.einsum(
        "bngk,bngv->bkgv", decayed_keys, value_block.astype(jnp.float32), precision=highest
    )
    new_state = jnp.exp(final_log)[:, None, :, None] * old_state + fresh
    new_state = new_state.reshape(sequences, HEAD, v_columns)
    retained = retained.reshape(tok_rows, groups, v_width)
    running = jnp.sum(retained, axis=-1)
    squares = jnp.sum(retained * retained, axis=-1)
    for bit_number in range(bit_count):
        other_sum, other_square = partner((running, squares), "mp", bit_number)
        running = running + other_sum
        squares = squares + other_square
    centre = running / VHEAD
    variance = squares / VHEAD - centre * centre
    deviation = retained - centre[..., None]
    normed = deviation * lax.rsqrt(variance + EPS)[..., None]
    gated_out = (normed.reshape(tok_rows, v_columns) * norm_gain * jax.nn.silu(gate_proj)).astype(
        jnp.bfloat16
    )
    partial_terms = jnp.dot(gated_out, w_out, preferred_element_type=jnp.float32)
    layer_out = lax.psum_scatter(partial_terms, "mp", scatter_dimension=1, tiled=True).astype(
        jnp.bfloat16
    )
    return (layer_out, new_state)


CHUNKS = 8
EXCHANGED = 2
TILE = 512
DEPTH = 8


def partners(device):
    core = device % 2
    across_x = device + 2 - 4 * ((device // 2) % 2)
    across_y = device + 4 - 8 * (device // 4)
    near = across_x + core * (across_y - across_x)
    far = across_y + core * (across_x - across_y)
    return near, far, across_x + across_y - device, device + 1 - 2 * core


def meet(devices):
    barrier = pltpu.get_barrier_semaphore()
    for device in devices:
        pl.semaphore_signal(
            barrier, inc=1, device_id={"mp": device}, device_id_type=pl.DeviceIdType.MESH
        )
    pl.semaphore_wait(barrier, len(devices))


def remote(source, target, send, recv, device):
    return pltpu.make_async_remote_copy(
        src_ref=source,
        dst_ref=target,
        send_sem=send,
        recv_sem=recv,
        device_id={"mp": device},
        device_id_type=pl.DeviceIdType.MESH,
    )


def fused_kernel(
    chunks,
    reduced,
    groups,
    tokens,
    w_query,
    w_key,
    w_value,
    w_gate,
    w_out,
    state,
    decay,
    gain,
    key_out,
    value_out,
    decay_out,
    layer_out,
    own_out,
    near_out,
    far_out,
    gathered,
    wq,
    wk,
    wv,
    wg,
    wo,
    q_held,
    k_held,
    v_held,
    g_held,
    s_held,
    gated,
    to_sibling,
    from_sibling,
    outgoing,
    incoming,
    total,
    parts,
    pending,
    finished,
    cumul,
    cumul_row,
    load_sem,
    state_sem,
    kv_sem,
    out_sem,
    send,
    recv,
    sum_send,
    sum_recv,
):
    me = lax.axis_index("mp")
    near, far, diagonal, sibling = partners(me)
    sib_near, sib_far, sib_diagonal, _ = partners(sibling)
    mine = (me, near, far, diagonal)
    theirs = (sibling, sib_near, sib_far, sib_diagonal)
    rows, width = tokens.shape
    size = rows // chunks
    sequences = size // NEW
    vw = w_value.shape[1] // groups

    def at(r):
        return pl.ds(pl.multiple_of(r * size, size), size)

    def span(device):
        return pl.ds(pl.multiple_of(device * width, width), width)

    def copy(lane, source, target, r):
        there = gathered.at[at(r), span(source)]
        return remote(there, there, send.at[lane, r], recv.at[lane, r], target)

    def swap(j, r):
        return remote(
            to_sibling.at[lax.rem(r, 2), j],
            from_sibling.at[j, at(r), :],
            sum_send.at[j, r],
            sum_recv.at[j, r],
            sibling,
        )

    def hop(lane, r):
        return remote(
            outgoing.at[lane, at(r), :],
            incoming.at[lane, at(r), :],
            sum_send.at[4 + lane, r],
            sum_recv.at[4 + lane, r],
            near if lane == 0 else far,
        )

    own = pltpu.make_async_copy(tokens, gathered.at[:, span(me)], load_sem.at[0])
    own.start()
    loads = [
        pltpu.make_async_copy(source, held, load_sem.at[1 + n])
        for n, (source, held) in enumerate(
            ((w_query, wq), (w_key, wk), (w_value, wv), (w_gate, wg), (w_out, wo))
        )
    ]
    for load in loads:
        load.start()

    def load_state(r):
        first = pl.multiple_of(r * sequences, sequences)
        return pltpu.make_async_copy(
            state.at[pl.ds(first, sequences)], s_held, state_sem.at[0]
        )

    def store_key(r):
        return pltpu.make_async_copy(
            k_held.at[lax.rem(r, 2)], key_out.at[at(r), :], kv_sem.at[0, r]
        )

    def store_value(r):
        return pltpu.make_async_copy(
            v_held.at[lax.rem(r, 2)], value_out.at[at(r), :], kv_sem.at[1, r]
        )

    def store_layer(r):
        return pltpu.make_async_copy(
            finished.at[at(r), :], layer_out.at[at(r), :], out_sem.at[0, r]
        )

    def store_shares(r):
        there = at(r - reduced)
        return [pltpu.make_async_copy(total.at[at(r), :], own_out.at[there, :], out_sem.at[0, r])] + [
            pltpu.make_async_copy(
                outgoing.at[lane, at(r), :], target.at[there, :], out_sem.at[1 + lane, r]
            )
            for lane, target in enumerate((near_out, far_out))
        ]

    meet((near, far, sibling))
    own.wait()

    def pass_near(r):
        copy(0, near, near, r).wait_recv()
        copy(2, near, far, r).start()
        copy(4, near, sibling, r).start()

    def pass_far(r):
        copy(1, far, far, r).wait_recv()
        copy(5, far, sibling, r).start()

    def pass_diagonal(r):
        copy(2, diagonal, far, r).wait_recv()
        copy(6, diagonal, sibling, r).start()

    def give_far(r):
        copy(1, me, far, r).start()
        copy(3, me, sibling, r).start()

    copy(0, me, near, 0).start()
    give_far(0)
    copy(0, me, near, 1).start()

    head = lax.broadcasted_iota(jnp.int32, (decay.shape[0], size), 0)
    token = lax.broadcasted_iota(jnp.int32, (8, size), 1) % NEW
    place = lax.broadcasted_iota(jnp.int32, (8, size), 0)

    def accumulate(r, carry):
        logs = jnp.log(decay[:, at(r)])
        sums = jnp.zeros((8, size), jnp.float32)
        for g in range(groups):
            chosen = jnp.where(head == me * groups + g, logs, 0.0)
            sums = jnp.where(place == g, jnp.sum(chosen, axis=0, keepdims=True), sums)
        shift = 1
        while shift < NEW:
            sums = sums + jnp.where(token >= shift, pltpu.roll(sums, shift, 1), 0.0)
            shift *= 2
        cumul_row[r] = sums
        cumul[at(r), :] = jnp.transpose(sums)
        return carry

    pass_near(0)
    give_far(1)
    copy(0, me, near, 2).start()
    pass_far(0)
    lax.fori_loop(0, chunks, accumulate, 0)
    decay_copy = pltpu.make_async_copy(cumul, decay_out, load_sem.at[6])
    decay_copy.start()
    pass_diagonal(0)
    pass_near(1)
    give_far(2)
    copy(0, me, near, 3).start()
    pass_far(1)
    give_far(3)

    place = lax.broadcasted_iota(jnp.int32, (size, size), 0)
    other = lax.broadcasted_iota(jnp.int32, (size, size), 1)
    causal = (place >= other) & (place // NEW == other // NEW)

    def project(r, weight, col, stop):
        return jnp.dot(
            gathered[at(r), :], weight[:, col:stop], preferred_element_type=jnp.float32
        )

    def share(dest):
        return jnp.dot(gated[...], wo[:, span(dest)], preferred_element_type=jnp.float32)

    def combine(r):
        slot = lax.rem(r, 2)
        for j in (3, 2, 1, 0):
            swap(j, r).wait_recv()
        for j in (3, 2, 1, 0):
            part = parts[slot, j] + from_sibling[j, at(r), :].astype(jnp.float32)
            if j >= 2:
                outgoing[j - 1, at(r), :] = part.astype(jnp.bfloat16)
            elif j == 1:
                pending[slot] = part
            else:
                total[at(r), :] = part
        hop(2, r).start()

        @pl.when(r < reduced)
        def _():
            hop(1, r).start()

    def relay(r):
        hop(2, r).wait_recv()
        part = pending[lax.rem(r, 2)] + incoming[2, at(r), :].astype(jnp.float32)
        outgoing[0, at(r), :] = part.astype(jnp.bfloat16)

        @pl.when(r < reduced)
        def _():
            hop(0, r).start()

        @pl.when(r >= reduced)
        def _():
            for store in store_shares(r):
                store.start()

    def finish(r):
        hop(1, r).wait_recv()
        hop(0, r).wait_recv()
        finished[at(r), :] = (
            total[at(r), :]
            + incoming[0, at(r), :].astype(jnp.float32)
            + incoming[1, at(r), :].astype(jnp.float32)
        ).astype(jnp.bfloat16)
        store_layer(r).start()

    def step(r, carry):
        slot = lax.rem(r, 2)
        load_state(r).start()

        @pl.when(r + 4 < chunks)
        def _():
            copy(0, me, near, r + 4).start()
            give_far(r + 4)

        for lane, source in ((3, sibling), (4, sib_near), (5, sib_far), (6, sib_diagonal)):
            copy(lane, source, sibling, r).wait_recv()

        @pl.when(r == 0)
        def _():
            for load in loads:
                load.wait()

        @pl.when(r >= 2)
        def _():
            store_key(r - 2).wait()
            store_value(r - 2).wait()
            for j in range(4):
                swap(j, r - 2).wait_send()

        for col in range(0, wq.shape[1], TILE):
            stop = min(col + TILE, wq.shape[1])
            q_held[:, col:stop] = (project(r, wq, col, stop) * HEAD ** (-0.5)).astype(jnp.bfloat16)
            k_held[slot, :, col:stop] = project(r, wk, col, stop).astype(jnp.bfloat16)
        for col in range(0, wv.shape[1], TILE):
            stop = min(col + TILE, wv.shape[1])
            v_held[slot, :, col:stop] = project(r, wv, col, stop).astype(jnp.bfloat16)
        for col in range(0, wg.shape[1], TILE):
            stop = min(col + TILE, wg.shape[1])
            gates = project(r, wg, col, stop)
            g_held[:, col:stop] = gain[:, col:stop] * (gates / (1.0 + jnp.exp(-gates)))

        store_key(r).start()
        store_value(r).start()

        @pl.when(r == 0)
        def _():
            pass_diagonal(1)
            pass_near(2)
            pass_far(2)

        @pl.when(r >= 2)
        def _():
            relay(r - 2)

        @pl.when(r >= 1)
        def _():
            combine(r - 1)

        @pl.when((r >= 4) & (r - 4 < reduced))
        def _():
            finish(r - 4)

        load_state(r).wait()
        for g in range(groups):
            vs = slice(g * vw, (g + 1) * vw)
            ks = slice(g * HEAD, (g + 1) * HEAD)
            query, key, value = q_held[:, ks], k_held[slot, :, ks], v_held[slot, :, vs]
            col = cumul[at(r), g : g + 1]
            row = cumul_row[r, g : g + 1, :]
            scores = lax.dot_general(
                query, key, (((1,), (1,)), ((), ())), preferred_element_type=jnp.float32
            )
            factor = jnp.where(causal, jnp.exp(jnp.where(causal, col - row, 0.0)), 0.0)
            weights = (scores * factor).astype(jnp.bfloat16)
            from_state = jnp.concatenate(
                [
                    jnp.dot(
                        query[s * NEW : (s + 1) * NEW],
                        s_held[s, :, vs].astype(jnp.bfloat16),
                        preferred_element_type=jnp.float32,
                    )
                    for s in range(sequences)
                ],
                axis=0,
            )
            in_block = jnp.dot(weights, value, preferred_element_type=jnp.float32)
            retained = jnp.exp(col) * from_state + in_block
            centre = jnp.mean(retained, axis=1, keepdims=True)
            deviation = retained - centre
            variance = jnp.mean(deviation * deviation, axis=1, keepdims=True)
            normed = deviation * lax.rsqrt(variance + EPS)
            gated[:, vs] = (normed * g_held[:, vs]).astype(jnp.bfloat16)

        for j in (3, 2, 1, 0):
            to_sibling[slot, j] = share(theirs[j]).astype(jnp.bfloat16)
        for j in (3, 2, 1, 0):
            parts[slot, j] = share(mine[j])
        for j in (3, 2, 1, 0):
            swap(j, r).start()

        @pl.when(r + 2 < chunks)
        def _():
            pass_diagonal(r + 2)

        @pl.when(r + 3 < chunks)
        def _():
            pass_near(r + 3)
            pass_far(r + 3)

        return carry

    lax.fori_loop(0, chunks, step, 0)
    combine(chunks - 1)
    relay(chunks - 2)
    relay(chunks - 1)
    for r in range(chunks - 4, reduced):
        finish(r)
    decay_copy.wait()

    def drain(r, carry):
        for lane, (source, target) in enumerate(
            (
                (me, near),
                (me, far),
                (near, far),
                (me, sibling),
                (near, sibling),
                (far, sibling),
                (diagonal, sibling),
            )
        ):
            copy(lane, source, target, r).wait_send()

        @pl.when(r >= chunks - 2)
        def _():
            store_key(r).wait()
            store_value(r).wait()
            for j in range(4):
                swap(j, r).wait_send()

        hop(2, r).wait_send()

        @pl.when(r < reduced)
        def _():
            for lane in range(2):
                hop(lane, r).wait_send()
            store_layer(r).wait()

        @pl.when(r >= reduced)
        def _():
            for store in store_shares(r):
                store.wait()

        return carry

    lax.fori_loop(0, chunks, drain, 0)


def fused(tokens, w_query, w_key, w_value, w_gate, w_out, state, decay, gain):
    rows, width = tokens.shape
    depth, qk = w_query.shape
    vc = w_value.shape[1]
    chunks, reduced = CHUNKS, EXCHANGED
    size = rows // chunks
    groups = qk // HEAD
    kept = reduced * size
    rest = rows - kept
    anywhere = pl.BlockSpec(memory_space=pl.ANY)
    vmem = pl.BlockSpec(memory_space=pltpu.VMEM)
    narrow = jnp.bfloat16
    wide = jnp.float32
    shapes = [
        ((rows, qk), narrow),
        ((rows, vc), narrow),
        ((rows, 8), wide),
        ((kept, width), narrow),
        ((rest, width), wide),
        ((rest, width), narrow),
        ((rest, width), narrow),
    ]
    return pl.pallas_call(
        functools.partial(fused_kernel, chunks, reduced, groups),
        in_specs=[anywhere] * 7 + [vmem] * 2,
        out_specs=[anywhere] * len(shapes),
        out_shape=[jax.ShapeDtypeStruct(*shape) for shape in shapes],
        scratch_shapes=[
            pltpu.VMEM((rows, depth), narrow),
            pltpu.VMEM((depth, qk), narrow),
            pltpu.VMEM((depth, qk), narrow),
            pltpu.VMEM((depth, vc), narrow),
            pltpu.VMEM((depth, vc), narrow),
            pltpu.VMEM(w_out.shape, narrow),
            pltpu.VMEM((size, qk), narrow),
            pltpu.VMEM((2, size, qk), narrow),
            pltpu.VMEM((2, size, vc), narrow),
            pltpu.VMEM((size, vc), wide),
            pltpu.VMEM((size // NEW,) + state.shape[1:], wide),
            pltpu.VMEM((size, vc), narrow),
            pltpu.VMEM((2, 4, size, width), narrow),
            pltpu.VMEM((4, rows, width), narrow),
            pltpu.VMEM((3, rows, width), narrow),
            pltpu.VMEM((3, rows, width), narrow),
            pltpu.VMEM((rows, width), wide),
            pltpu.VMEM((2, 4, size, width), wide),
            pltpu.VMEM((2, size, width), wide),
            pltpu.VMEM((kept, width), narrow),
            pltpu.VMEM((rows, 8), wide),
            pltpu.VMEM((chunks, 8, size), wide),
            pltpu.SemaphoreType.DMA((7,)),
            pltpu.SemaphoreType.DMA((1,)),
            pltpu.SemaphoreType.DMA((2, chunks)),
            pltpu.SemaphoreType.DMA((4, chunks)),
            pltpu.SemaphoreType.DMA((7, chunks)),
            pltpu.SemaphoreType.DMA((7, chunks)),
            pltpu.SemaphoreType.DMA((7, chunks)),
            pltpu.SemaphoreType.DMA((7, chunks)),
        ],
        compiler_params=pltpu.CompilerParams(
            collective_id=0, has_side_effects=True, vmem_limit_bytes=67043328
        ),
        cost_estimate=pl.CostEstimate(
            flops=2 * rows * depth * (2 * qk + 3 * vc),
            bytes_accessed=4 * state.size,
            transcendentals=rows * vc,
        ),
    )(tokens, w_query, w_key, w_value, w_gate, w_out, state, decay, gain)


def update_kernel(
    groups,
    c_col,
    k,
    v,
    state,
    new_state,
    c_held,
    k_held,
    v_held,
    s_in,
    s_out,
    load_sem,
    in_sem,
    out_sem,
):
    vw = v.shape[1] // groups
    sequences = state.shape[0]
    depth = s_in.shape[0]

    def load(s):
        slot = lax.rem(s, depth)
        return pltpu.make_async_copy(state.at[s], s_in.at[slot], in_sem.at[slot])

    def store(s):
        slot = lax.rem(s, depth)
        return pltpu.make_async_copy(s_out.at[slot], new_state.at[s], out_sem.at[slot])

    rows = [
        pltpu.make_async_copy(source, held, load_sem.at[n])
        for n, (source, held) in enumerate(((c_col, c_held), (k, k_held), (v, v_held)))
    ]
    for copy in rows:
        copy.start()

    def fill(s, carry):
        load(s).start()
        return carry

    lax.fori_loop(0, depth, fill, 0)
    for copy in rows:
        copy.wait()

    def step(s, carry):
        slot = lax.rem(s, depth)
        load(s).wait()

        @pl.when(s >= depth)
        def _():
            store(s - depth).wait()

        at = pl.ds(pl.multiple_of(s * NEW, NEW), NEW)
        for g in range(groups):
            vs = slice(g * vw, (g + 1) * vw)
            col = c_held[at, g : g + 1]
            last = col[NEW - 1 : NEW, :]
            key = k_held[at, g * HEAD : (g + 1) * HEAD].astype(jnp.float32)
            scaled = (key * jnp.exp(last - col)).astype(jnp.bfloat16)
            fresh = lax.dot_general(
                scaled,
                v_held[at, vs],
                (((0,), (0,)), ((), ())),
                preferred_element_type=jnp.float32,
            )
            s_out[slot, :, vs] = jnp.exp(last) * s_in[slot, :, vs] + fresh
        store(s).start()

        @pl.when(s + depth < sequences)
        def _():
            load(s + depth).start()

        return carry

    lax.fori_loop(0, sequences, step, 0)

    def drain(s, carry):
        store(sequences - depth + s).wait()
        return carry

    lax.fori_loop(0, depth, drain, 0)


def update_state(groups, c_col, k, v, state):
    rows = c_col.shape[0]
    depth = min(DEPTH, state.shape[0])
    anywhere = pl.BlockSpec(memory_space=pl.ANY)
    return pl.pallas_call(
        functools.partial(update_kernel, groups),
        in_specs=[anywhere] * 4,
        out_specs=anywhere,
        out_shape=jax.ShapeDtypeStruct(state.shape, jnp.float32),
        scratch_shapes=[
            pltpu.VMEM(c_col.shape, jnp.float32),
            pltpu.VMEM(k.shape, k.dtype),
            pltpu.VMEM(v.shape, v.dtype),
            pltpu.VMEM((depth,) + state.shape[1:], jnp.float32),
            pltpu.VMEM((depth,) + state.shape[1:], jnp.float32),
            pltpu.SemaphoreType.DMA((3,)),
            pltpu.SemaphoreType.DMA((depth,)),
            pltpu.SemaphoreType.DMA((depth,)),
        ],
        compiler_params=pltpu.CompilerParams(vmem_limit_bytes=60 << 20),
        cost_estimate=pl.CostEstimate(
            flops=2 * rows * HEAD * v.shape[1],
            bytes_accessed=8 * state.size,
            transcendentals=rows,
        ),
    )(c_col, k, v, state)


def whole_heads(tokens, decay, state, w_query, w_key, w_value, w_gate, w_out, norm_gain):
    groups = w_query.shape[1] // HEAD
    key_proj, value_proj, cumul, reduced, own, *shares = fused(
        tokens,
        w_query,
        w_key,
        w_value,
        w_gate,
        w_out,
        state,
        decay.T,
        norm_gain.reshape(1, -1),
    )
    devices = range(lax.axis_size("mp"))
    for n, share in enumerate(shares):
        pairs = [(device, partners(device)[n]) for device in devices]
        own = own + lax.ppermute(share, "mp", pairs).astype(jnp.float32)
    layer_out = jnp.concatenate([reduced, own.astype(jnp.bfloat16)])
    return (layer_out, update_state(groups, cumul, key_proj, value_proj, state))


def per_device(tokens, decay, state, w_query, *rest):
    whole = w_query.shape[1] % HEAD == 0 and lax.axis_size("mp") == 8
    path = whole_heads if whole else split_heads
    return path(tokens, decay, state, w_query, *rest)


def solution(mesh):
    placed = (
        P("dp", "mp"),
        P("dp", None),
        P("dp", None, "mp"),
        P(None, "mp"),
        P(None, "mp"),
        P(None, "mp"),
        P(None, "mp"),
        P("mp", None),
        P("mp"),
    )
    return jax.shard_map(
        per_device,
        mesh=mesh,
        in_specs=placed,
        out_specs=(P("dp", "mp"), P("dp", None, "mp")),
        check_vma=False,
    )
```

```python
import functools

import jax
import jax.numpy as jnp
from jax import lax
from jax.experimental import pallas as pl
from jax.experimental.pallas import tpu as pltpu
from jax.sharding import PartitionSpec as P

HEAD = 256
VHEAD = 512
NEW = 32


EPS = 0.1


def partner(shard, axis, bit):
    return lax.ppermute(shard, axis, [(i, i ^ 1 << bit) for i in range(lax.axis_size(axis))])


def split_heads(tokens, decay, state, w_query, w_key, w_value, w_gate, w_out, norm_gain):
    highest = lax.Precision.HIGHEST
    tok_rows = tokens.shape[0]
    qk_columns = w_query.shape[1]
    v_columns = w_value.shape[1]
    head_span = max(1, HEAD // qk_columns)
    groups = max(1, qk_columns // HEAD)
    qk_width = qk_columns // groups
    v_width = v_columns // groups
    sequences = tok_rows // NEW
    bit_count = head_span.bit_length() - 1
    device_index = lax.axis_index("mp")
    first_head = device_index * qk_columns // HEAD
    qk_zeros = jnp.zeros((tok_rows, qk_columns), jnp.float32)
    v_zeros = jnp.zeros((tok_rows, v_columns), jnp.float32)
    carried = (qk_zeros, qk_zeros, v_zeros, v_zeros)
    segment = lax.all_gather(tokens, "mp", axis=1, tiled=True)
    updated = []
    for running, weight in zip(carried, (w_query, w_key, w_value, w_gate)):
        updated.append(jnp.dot(segment, weight, preferred_element_type=jnp.float32))
    query, key_proj, value_proj, gate_proj = tuple(updated)
    query = (query * HEAD ** (-0.5)).astype(jnp.bfloat16).reshape(tok_rows, groups, qk_width)
    key_proj = key_proj.astype(jnp.bfloat16).reshape(tok_rows, groups, qk_width)
    value_proj = value_proj.astype(jnp.bfloat16)
    for bit_number in range(bit_count):
        other_query, other_key = partner((query, key_proj), "mp", bit_number)
        upper_half = device_index >> bit_number & 1 == 1
        query = jnp.where(
            upper_half,
            jnp.concatenate([other_query, query], 2),
            jnp.concatenate([query, other_query], 2),
        )
        key_proj = jnp.where(
            upper_half,
            jnp.concatenate([other_key, key_proj], 2),
            jnp.concatenate([key_proj, other_key], 2),
        )
    query_block = query.reshape(sequences, NEW, groups, HEAD)
    key_block = key_proj.reshape(sequences, NEW, groups, HEAD)
    value_block = value_proj.reshape(sequences, NEW, groups, v_width)
    decay_rates = lax.dynamic_slice_in_dim(decay, first_head, groups, 1).reshape(
        sequences, NEW, groups
    )
    log_cumul = jnp.cumsum(jnp.log(decay_rates), axis=1)
    old_state = state.reshape(sequences, HEAD, groups, v_width)
    from_state = jnp.einsum(
        "bngk,bkgv->bngv", query_block.astype(jnp.float32), old_state, precision=highest
    )
    scores = jnp.einsum(
        "bngk,bmgk->bgnm", query_block, key_block, preferred_element_type=jnp.float32
    )
    along = jnp.transpose(log_cumul, (0, 2, 1))
    log_gap = along[:, :, :, None] - along[:, :, None, :]
    causal = jnp.arange(NEW)[:, None] >= jnp.arange(NEW)[None, :]
    factor = jnp.where(causal, jnp.exp(jnp.where(causal, log_gap, 0.0)), 0.0)
    weights = (scores * factor).astype(jnp.bfloat16)
    in_block = jnp.einsum(
        "bgnm,bmgv->bngv", weights, value_block, preferred_element_type=jnp.float32
    )
    retained = jnp.exp(log_cumul)[..., None] * from_state + in_block
    final_log = log_cumul[:, -1, :]
    carry_scale = jnp.exp(final_log[:, None, :] - log_cumul)
    decayed_keys = key_block.astype(jnp.float32) * carry_scale[..., None]
    fresh = jnp.einsum(
        "bngk,bngv->bkgv", decayed_keys, value_block.astype(jnp.float32), precision=highest
    )
    new_state = jnp.exp(final_log)[:, None, :, None] * old_state + fresh
    new_state = new_state.reshape(sequences, HEAD, v_columns)
    retained = retained.reshape(tok_rows, groups, v_width)
    running = jnp.sum(retained, axis=-1)
    squares = jnp.sum(retained * retained, axis=-1)
    for bit_number in range(bit_count):
        other_sum, other_square = partner((running, squares), "mp", bit_number)
        running = running + other_sum
        squares = squares + other_square
    centre = running / VHEAD
    variance = squares / VHEAD - centre * centre
    deviation = retained - centre[..., None]
    normed = deviation * lax.rsqrt(variance + EPS)[..., None]
    gated_out = (normed.reshape(tok_rows, v_columns) * norm_gain * jax.nn.silu(gate_proj)).astype(
        jnp.bfloat16
    )
    partial_terms = jnp.dot(gated_out, w_out, preferred_element_type=jnp.float32)
    layer_out = lax.psum_scatter(partial_terms, "mp", scatter_dimension=1, tiled=True).astype(
        jnp.bfloat16
    )
    return (layer_out, new_state)


CHUNKS = 8
TILE = 512
DEPTH = 8


def partners(device):
    core = device % 2
    across_x = device + 2 - 4 * ((device // 2) % 2)
    across_y = device + 4 - 8 * (device // 4)
    near = across_x + core * (across_y - across_x)
    far = across_y + core * (across_x - across_y)
    return near, far, across_x + across_y - device, device + 1 - 2 * core


def meet(devices):
    barrier = pltpu.get_barrier_semaphore()
    for device in devices:
        pl.semaphore_signal(
            barrier, inc=1, device_id={"mp": device}, device_id_type=pl.DeviceIdType.MESH
        )
    pl.semaphore_wait(barrier, len(devices))


def remote(source, target, send, recv, device):
    return pltpu.make_async_remote_copy(
        src_ref=source,
        dst_ref=target,
        send_sem=send,
        recv_sem=recv,
        device_id={"mp": device},
        device_id_type=pl.DeviceIdType.MESH,
    )


def fused_kernel(
    chunks,
    groups,
    tokens,
    w_query,
    w_key,
    w_value,
    w_gate,
    w_out,
    state,
    decay,
    gain,
    key_out,
    value_out,
    decay_out,
    own_out,
    near_out,
    far_out,
    gathered,
    wq,
    wk,
    wv,
    wg,
    wo,
    q_held,
    k_held,
    v_held,
    g_held,
    s_held,
    gated,
    to_sibling,
    from_sibling,
    outgoing,
    incoming,
    total,
    parts,
    pending,
    cumul,
    cumul_row,
    load_sem,
    state_sem,
    kv_sem,
    out_sem,
    send,
    recv,
    sum_send,
    sum_recv,
):
    me = lax.axis_index("mp")
    near, far, diagonal, sibling = partners(me)
    sib_near, sib_far, sib_diagonal, _ = partners(sibling)
    mine = (me, near, far, diagonal)
    theirs = (sibling, sib_near, sib_far, sib_diagonal)
    rows, width = tokens.shape
    size = rows // chunks
    sequences = size // NEW
    vw = w_value.shape[1] // groups

    def at(r):
        return pl.ds(pl.multiple_of(r * size, size), size)

    def span(device):
        return pl.ds(pl.multiple_of(device * width, width), width)

    def copy(lane, source, target, r):
        there = gathered.at[at(r), span(source)]
        return remote(there, there, send.at[lane, r], recv.at[lane, r], target)

    def swap(j, r):
        return remote(
            to_sibling.at[lax.rem(r, 2), j],
            from_sibling.at[j, at(r), :],
            sum_send.at[j, r],
            sum_recv.at[j, r],
            sibling,
        )

    def hop(r):
        return remote(
            outgoing.at[2, at(r), :],
            incoming.at[at(r), :],
            sum_send.at[4, r],
            sum_recv.at[4, r],
            far,
        )

    own = pltpu.make_async_copy(tokens, gathered.at[:, span(me)], load_sem.at[0])
    own.start()
    loads = [
        pltpu.make_async_copy(source, held, load_sem.at[1 + n])
        for n, (source, held) in enumerate(
            ((w_query, wq), (w_key, wk), (w_value, wv), (w_gate, wg), (w_out, wo))
        )
    ]
    for load in loads:
        load.start()

    def load_state(r):
        first = pl.multiple_of(r * sequences, sequences)
        return pltpu.make_async_copy(
            state.at[pl.ds(first, sequences)], s_held, state_sem.at[0]
        )

    def store_key(r):
        return pltpu.make_async_copy(
            k_held.at[lax.rem(r, 2)], key_out.at[at(r), :], kv_sem.at[0, r]
        )

    def store_value(r):
        return pltpu.make_async_copy(
            v_held.at[lax.rem(r, 2)], value_out.at[at(r), :], kv_sem.at[1, r]
        )

    def store_shares(r):
        return [
            pltpu.make_async_copy(source.at[at(r), :], target.at[at(r), :], out_sem.at[n, r])
            for n, (source, target) in enumerate(
                ((total, own_out), (outgoing.at[0], near_out), (outgoing.at[1], far_out))
            )
        ]

    meet((near, far, sibling))
    own.wait()

    def pass_near(r):
        copy(0, near, near, r).wait_recv()
        copy(2, near, far, r).start()
        copy(4, near, sibling, r).start()

    def pass_far(r):
        copy(1, far, far, r).wait_recv()
        copy(5, far, sibling, r).start()

    def pass_diagonal(r):
        copy(2, diagonal, far, r).wait_recv()
        copy(6, diagonal, sibling, r).start()

    def give_far(r):
        copy(1, me, far, r).start()
        copy(3, me, sibling, r).start()

    copy(0, me, near, 0).start()
    give_far(0)
    copy(0, me, near, 1).start()

    head = lax.broadcasted_iota(jnp.int32, (decay.shape[0], size), 0)
    token = lax.broadcasted_iota(jnp.int32, (8, size), 1) % NEW
    place = lax.broadcasted_iota(jnp.int32, (8, size), 0)

    def accumulate(r, carry):
        logs = jnp.log(decay[:, at(r)])
        sums = jnp.zeros((8, size), jnp.float32)
        for g in range(groups):
            chosen = jnp.where(head == me * groups + g, logs, 0.0)
            sums = jnp.where(place == g, jnp.sum(chosen, axis=0, keepdims=True), sums)
        shift = 1
        while shift < NEW:
            sums = sums + jnp.where(token >= shift, pltpu.roll(sums, shift, 1), 0.0)
            shift *= 2
        cumul_row[r] = sums
        cumul[at(r), :] = jnp.transpose(sums)
        return carry

    pass_near(0)
    give_far(1)
    copy(0, me, near, 2).start()
    pass_far(0)
    lax.fori_loop(0, chunks, accumulate, 0)
    decay_copy = pltpu.make_async_copy(cumul, decay_out, load_sem.at[6])
    decay_copy.start()
    pass_diagonal(0)
    pass_near(1)
    give_far(2)
    copy(0, me, near, 3).start()
    pass_far(1)
    give_far(3)

    place = lax.broadcasted_iota(jnp.int32, (size, size), 0)
    other = lax.broadcasted_iota(jnp.int32, (size, size), 1)
    causal = (place >= other) & (place // NEW == other // NEW)

    def project(r, weight, col, stop):
        return jnp.dot(
            gathered[at(r), :], weight[:, col:stop], preferred_element_type=jnp.float32
        )

    def share(dest):
        return jnp.dot(gated[...], wo[:, span(dest)], preferred_element_type=jnp.float32)

    def combine(r):
        slot = lax.rem(r, 2)
        for j in (3, 2, 1, 0):
            swap(j, r).wait_recv()
        for j in (3, 2, 1, 0):
            part = parts[slot, j] + from_sibling[j, at(r), :].astype(jnp.float32)
            if j >= 2:
                outgoing[j - 1, at(r), :] = part.astype(jnp.bfloat16)
                if j == 3:
                    hop(r).start()
            elif j == 1:
                pending[slot] = part
            else:
                total[at(r), :] = part

    def relay(r):
        hop(r).wait_recv()
        part = pending[lax.rem(r, 2)] + incoming[at(r), :].astype(jnp.float32)
        outgoing[0, at(r), :] = part.astype(jnp.bfloat16)
        for store in store_shares(r):
            store.start()

    def step(r, carry):
        slot = lax.rem(r, 2)
        load_state(r).start()
        for lane, source in ((3, sibling), (4, sib_near), (5, sib_far), (6, sib_diagonal)):
            copy(lane, source, sibling, r).wait_recv()

        @pl.when(r == 0)
        def _():
            for load in loads:
                load.wait()

        @pl.when(r >= 2)
        def _():
            store_key(r - 2).wait()
            store_value(r - 2).wait()
            for j in range(4):
                swap(j, r - 2).wait_send()

        for col in range(0, wq.shape[1], TILE):
            stop = min(col + TILE, wq.shape[1])
            q_held[:, col:stop] = (project(r, wq, col, stop) * HEAD ** (-0.5)).astype(jnp.bfloat16)
            k_held[slot, :, col:stop] = project(r, wk, col, stop).astype(jnp.bfloat16)
        for col in range(0, wv.shape[1], TILE):
            stop = min(col + TILE, wv.shape[1])
            v_held[slot, :, col:stop] = project(r, wv, col, stop).astype(jnp.bfloat16)
        for col in range(0, wg.shape[1], TILE):
            stop = min(col + TILE, wg.shape[1])
            gates = project(r, wg, col, stop)
            g_held[:, col:stop] = gain[:, col:stop] * (gates / (1.0 + jnp.exp(-gates)))

        store_key(r).start()
        store_value(r).start()

        @pl.when(r + 1 < chunks)
        def _():
            pass_diagonal(r + 1)

        @pl.when(r + 2 < chunks)
        def _():
            pass_near(r + 2)
            pass_far(r + 2)

        @pl.when(r + 4 < chunks)
        def _():
            copy(0, me, near, r + 4).start()
            give_far(r + 4)

        @pl.when(r >= 2)
        def _():
            relay(r - 2)

        @pl.when(r >= 1)
        def _():
            combine(r - 1)

        load_state(r).wait()
        for g in range(groups):
            vs = slice(g * vw, (g + 1) * vw)
            ks = slice(g * HEAD, (g + 1) * HEAD)
            query, key, value = q_held[:, ks], k_held[slot, :, ks], v_held[slot, :, vs]
            col = cumul[at(r), g : g + 1]
            row = cumul_row[r, g : g + 1, :]
            scores = lax.dot_general(
                query, key, (((1,), (1,)), ((), ())), preferred_element_type=jnp.float32
            )
            factor = jnp.where(causal, jnp.exp(jnp.where(causal, col - row, 0.0)), 0.0)
            weights = (scores * factor).astype(jnp.bfloat16)
            from_state = jnp.concatenate(
                [
                    jnp.dot(
                        query[s * NEW : (s + 1) * NEW],
                        s_held[s, :, vs].astype(jnp.bfloat16),
                        preferred_element_type=jnp.float32,
                    )
                    for s in range(sequences)
                ],
                axis=0,
            )
            in_block = jnp.dot(weights, value, preferred_element_type=jnp.float32)
            retained = jnp.exp(col) * from_state + in_block
            centre = jnp.mean(retained, axis=1, keepdims=True)
            deviation = retained - centre
            variance = jnp.mean(deviation * deviation, axis=1, keepdims=True)
            normed = deviation * lax.rsqrt(variance + EPS)
            gated[:, vs] = (normed * g_held[:, vs]).astype(jnp.bfloat16)

        for j in (3, 2, 1, 0):
            to_sibling[slot, j] = share(theirs[j]).astype(jnp.bfloat16)
        for j in (3, 2, 1, 0):
            parts[slot, j] = share(mine[j])
        for j in (3, 2, 1, 0):
            swap(j, r).start()

        return carry

    lax.fori_loop(0, chunks, step, 0)
    combine(chunks - 1)
    relay(chunks - 2)
    relay(chunks - 1)
    decay_copy.wait()

    def drain(r, carry):
        for lane, (source, target) in enumerate(
            (
                (me, near),
                (me, far),
                (near, far),
                (me, sibling),
                (near, sibling),
                (far, sibling),
                (diagonal, sibling),
            )
        ):
            copy(lane, source, target, r).wait_send()

        @pl.when(r >= chunks - 2)
        def _():
            store_key(r).wait()
            store_value(r).wait()
            for j in range(4):
                swap(j, r).wait_send()

        hop(r).wait_send()
        for store in store_shares(r):
            store.wait()
        return carry

    lax.fori_loop(0, chunks, drain, 0)


def fused(tokens, w_query, w_key, w_value, w_gate, w_out, state, decay, gain):
    rows, width = tokens.shape
    depth, qk = w_query.shape
    vc = w_value.shape[1]
    chunks = CHUNKS
    size = rows // chunks
    groups = qk // HEAD
    anywhere = pl.BlockSpec(memory_space=pl.ANY)
    vmem = pl.BlockSpec(memory_space=pltpu.VMEM)
    narrow = jnp.bfloat16
    wide = jnp.float32
    shapes = [
        ((rows, qk), narrow),
        ((rows, vc), narrow),
        ((rows, 8), wide),
        ((rows, width), wide),
        ((rows, width), narrow),
        ((rows, width), narrow),
    ]
    return pl.pallas_call(
        functools.partial(fused_kernel, chunks, groups),
        in_specs=[anywhere] * 7 + [vmem] * 2,
        out_specs=[anywhere] * len(shapes),
        out_shape=[jax.ShapeDtypeStruct(*shape) for shape in shapes],
        scratch_shapes=[
            pltpu.VMEM((rows, depth), narrow),
            pltpu.VMEM((depth, qk), narrow),
            pltpu.VMEM((depth, qk), narrow),
            pltpu.VMEM((depth, vc), narrow),
            pltpu.VMEM((depth, vc), narrow),
            pltpu.VMEM(w_out.shape, narrow),
            pltpu.VMEM((size, qk), narrow),
            pltpu.VMEM((2, size, qk), narrow),
            pltpu.VMEM((2, size, vc), narrow),
            pltpu.VMEM((size, vc), wide),
            pltpu.VMEM((size // NEW,) + state.shape[1:], wide),
            pltpu.VMEM((size, vc), narrow),
            pltpu.VMEM((2, 4, size, width), narrow),
            pltpu.VMEM((4, rows, width), narrow),
            pltpu.VMEM((3, rows, width), narrow),
            pltpu.VMEM((rows, width), narrow),
            pltpu.VMEM((rows, width), wide),
            pltpu.VMEM((2, 4, size, width), wide),
            pltpu.VMEM((2, size, width), wide),
            pltpu.VMEM((rows, 8), wide),
            pltpu.VMEM((chunks, 8, size), wide),
            pltpu.SemaphoreType.DMA((7,)),
            pltpu.SemaphoreType.DMA((1,)),
            pltpu.SemaphoreType.DMA((2, chunks)),
            pltpu.SemaphoreType.DMA((3, chunks)),
            pltpu.SemaphoreType.DMA((7, chunks)),
            pltpu.SemaphoreType.DMA((7, chunks)),
            pltpu.SemaphoreType.DMA((5, chunks)),
            pltpu.SemaphoreType.DMA((5, chunks)),
        ],
        compiler_params=pltpu.CompilerParams(
            collective_id=0, has_side_effects=True, vmem_limit_bytes=67043328
        ),
        cost_estimate=pl.CostEstimate(
            flops=2 * rows * depth * (2 * qk + 3 * vc),
            bytes_accessed=4 * state.size,
            transcendentals=rows * vc,
        ),
    )(tokens, w_query, w_key, w_value, w_gate, w_out, state, decay, gain)


def update_kernel(
    groups,
    c_col,
    k,
    v,
    state,
    new_state,
    c_held,
    k_held,
    v_held,
    s_in,
    s_out,
    load_sem,
    in_sem,
    out_sem,
):
    vw = v.shape[1] // groups
    sequences = state.shape[0]
    depth = s_in.shape[0]

    def load(s):
        slot = lax.rem(s, depth)
        return pltpu.make_async_copy(state.at[s], s_in.at[slot], in_sem.at[slot])

    def store(s):
        slot = lax.rem(s, depth)
        return pltpu.make_async_copy(s_out.at[slot], new_state.at[s], out_sem.at[slot])

    rows = [
        pltpu.make_async_copy(source, held, load_sem.at[n])
        for n, (source, held) in enumerate(((c_col, c_held), (k, k_held), (v, v_held)))
    ]
    for copy in rows:
        copy.start()

    def fill(s, carry):
        load(s).start()
        return carry

    lax.fori_loop(0, depth, fill, 0)
    for copy in rows:
        copy.wait()

    def step(s, carry):
        slot = lax.rem(s, depth)
        load(s).wait()

        @pl.when(s >= depth)
        def _():
            store(s - depth).wait()

        at = pl.ds(pl.multiple_of(s * NEW, NEW), NEW)
        for g in range(groups):
            vs = slice(g * vw, (g + 1) * vw)
            col = c_held[at, g : g + 1]
            last = col[NEW - 1 : NEW, :]
            key = k_held[at, g * HEAD : (g + 1) * HEAD].astype(jnp.float32)
            scaled = (key * jnp.exp(last - col)).astype(jnp.bfloat16)
            fresh = lax.dot_general(
                scaled,
                v_held[at, vs],
                (((0,), (0,)), ((), ())),
                preferred_element_type=jnp.float32,
            )
            s_out[slot, :, vs] = jnp.exp(last) * s_in[slot, :, vs] + fresh
        store(s).start()

        @pl.when(s + depth < sequences)
        def _():
            load(s + depth).start()

        return carry

    lax.fori_loop(0, sequences, step, 0)

    def drain(s, carry):
        store(sequences - depth + s).wait()
        return carry

    lax.fori_loop(0, depth, drain, 0)


def update_state(groups, c_col, k, v, state):
    rows = c_col.shape[0]
    depth = min(DEPTH, state.shape[0])
    anywhere = pl.BlockSpec(memory_space=pl.ANY)
    return pl.pallas_call(
        functools.partial(update_kernel, groups),
        in_specs=[anywhere] * 4,
        out_specs=anywhere,
        out_shape=jax.ShapeDtypeStruct(state.shape, jnp.float32),
        scratch_shapes=[
            pltpu.VMEM(c_col.shape, jnp.float32),
            pltpu.VMEM(k.shape, k.dtype),
            pltpu.VMEM(v.shape, v.dtype),
            pltpu.VMEM((depth,) + state.shape[1:], jnp.float32),
            pltpu.VMEM((depth,) + state.shape[1:], jnp.float32),
            pltpu.SemaphoreType.DMA((3,)),
            pltpu.SemaphoreType.DMA((depth,)),
            pltpu.SemaphoreType.DMA((depth,)),
        ],
        compiler_params=pltpu.CompilerParams(vmem_limit_bytes=60 << 20),
        cost_estimate=pl.CostEstimate(
            flops=2 * rows * HEAD * v.shape[1],
            bytes_accessed=8 * state.size,
            transcendentals=rows,
        ),
    )(c_col, k, v, state)


def whole_heads(tokens, decay, state, w_query, w_key, w_value, w_gate, w_out, norm_gain):
    groups = w_query.shape[1] // HEAD
    key_proj, value_proj, cumul, own, *shares = fused(
        tokens,
        w_query,
        w_key,
        w_value,
        w_gate,
        w_out,
        state,
        decay.T,
        norm_gain.reshape(1, -1),
    )
    devices = range(lax.axis_size("mp"))
    for n, share in enumerate(shares):
        pairs = [(device, partners(device)[n]) for device in devices]
        own = own + lax.ppermute(share, "mp", pairs).astype(jnp.float32)
    return (own.astype(jnp.bfloat16), update_state(groups, cumul, key_proj, value_proj, state))


def per_device(tokens, decay, state, w_query, *rest):
    whole = w_query.shape[1] % HEAD == 0 and lax.axis_size("mp") == 8
    path = whole_heads if whole else split_heads
    return path(tokens, decay, state, w_query, *rest)


def solution(mesh):
    placed = (
        P("dp", "mp"),
        P("dp", None),
        P("dp", None, "mp"),
        P(None, "mp"),
        P(None, "mp"),
        P(None, "mp"),
        P(None, "mp"),
        P("mp", None),
        P("mp"),
    )
    return jax.shard_map(
        per_device,
        mesh=mesh,
        in_specs=placed,
        out_specs=(P("dp", "mp"), P("dp", None, "mp")),
        check_vma=False,
    )
```
